32 devices in a mesh: grp: 2 (over x), seq: 16 (over z, y, core).
Axes of the slice: x: 2, y: 2, z: 4, core: 2. Of those that a mesh axis runs over, the one named last changes fastest.
Arguments:
- item_features: bfloat16 [4096, 1024], P(('grp', 'seq')), parts along dimension 0, may hold values from -6 to 6
- tower_in: bfloat16 [1024, 2048], replicated, may hold values from -0.1875 to 0.1875
- tower_out: bfloat16 [2048, 512], replicated, may hold values from -0.125 to 0.125
- proj_weight: bfloat16 [512, 2048], replicated, may hold values from -0.25 to 0.25
- out_weight: bfloat16 [512, 512], replicated, may hold values from -0.25 to 0.25
- hist_keys: bfloat16 [4, 16384, 512], P('grp', 'seq'), parts along dimension 0, may hold values from -6 to 6
- hist_values: bfloat16 [4, 16384, 512], P('grp', 'seq'), parts along dimension 0, may hold values from -6 to 6
- owner_of: int32 [512, 2, 1], P(('grp', 'seq')), parts along dimension 0, may hold values from 0 to 15; in each aligned block of 32 rows (0 to 31, 32 to 63, ..., all dimensions but the last counted through in order) at most 4 rows name the same one
- row_in: int32 [512, 2], P(('grp', 'seq')), parts along dimension 0, may hold values from 0 to 127
- hist_lengths: int32 [4], P('grp'), parts along dimension 0, may hold values from 4096 to 16384
- causal_offsets: int32 [512, 2], P('grp'), parts along dimension 0, may hold values from 0 to 1023
Outputs:
- item_embed: bfloat16 [4096, 512], P(('grp', 'seq')), parts along dimension 0
- cand_out: bfloat16 [512, 2, 512], P(('grp', 'seq')), parts along dimension 0
The draws below stay inside these ranges and needn't reach their ends.
There are 2 independent parts, one for each index of `grp`. The reference program is written for one: setup_inputs(seed, part) draws one part's arguments, and reference() takes and returns one part's arrays. A program takes and returns all parts, laid end to end along the dimension named above; an argument that names none is the same for every part. Nothing has to cross between parts.
Inputs may be any that keep to these rules, and one draw needn't show every extreme that they name: `owner_of`: within the 32 slots of one device (candidate-major), no device number appears more than 4 times.
All inputs are finite; a program needn't handle non-finite values.
Results may differ from the reference program's by a relative error of at most 0.011.
Values may be sent and summed in bfloat16 or wider, within the bound.
A program may use at most 128 MiB of HBM per device.

```python
import math
import jax
import jax.numpy as jnp
import numpy as np
from jax import lax

D = 512
FEAT = 1024
TOWER = 2048
HEADS = 8
USERS = 2
CAND_DEV = 128
CPS_DEV = 16
HIST_DEV = 1024
CAND = 2048
CPS = 256
HIST = 16384
MOST = 4
N_SEQ = 16


def with_ends(drawn, own_key, least, largest):
    longest = drawn.shape.index(max(drawn.shape))
    spots = []
    for shift in (0, 1):
        where = [jax.random.randint(jax.random.fold_in(own_key, axis), (), 0, length) for axis, length in enumerate(drawn.shape)]
        where[longest] = (where[longest] + shift) % drawn.shape[longest]
        spots.append(tuple(where))
    return drawn.at[spots[0]].set(least).at[spots[1]].set(largest)


def block_scale(key, dims, split, low, high):
    gain, own = 1.0, jax.random.fold_in(key, 6)
    for dim, blocks in split:
        draws = jnp.exp(jax.random.uniform(jax.random.fold_in(own, dim), (blocks,), jnp.float32, low / len(split), high / len(split)))
        gain = gain * jnp.repeat(draws, dims[dim] // blocks).reshape([-1 if axis == dim else 1 for axis in range(len(dims))])
    return gain


def assign_block(key, own, number, rows, number_of, top, most, slope):
    order = jax.random.permutation(key, number_of)
    crowded, ordinary = portions_of(number_of, rows * top, most, slope, True), portions_of(number_of, rows * top, most, slope, False)
    places = jnp.arange(number_of)

    def named(lengths, turn):
        used = int((lengths > 0).sum())
        fixed = max(1, used // 4)
        moved = fixed + (places - fixed + turn * (used - fixed)) % max(1, number_of - fixed)
        return jnp.zeros((number_of,), jnp.int32).at[order[jnp.where(places < fixed, places, moved)]].set(jnp.asarray(lengths, jnp.int32))

    lengths = jnp.where(number % 4 == 0, named(crowded, number // 4), named(ordinary, number - number // 4 - 1))
    mixed = jax.random.permutation(jax.random.fold_in(own, 3), number_of)
    giver, receiver = mixed[0:number_of // 2 * 2:2], mixed[1:number_of // 2 * 2:2]
    room = jnp.minimum(lengths[giver] - 1, most - lengths[receiver]) // 2
    room = jnp.where((giver == order[0]) | (receiver == order[0]) | (lengths[receiver] == 0), 0, jnp.maximum(room, 0))
    moved = jax.random.randint(jax.random.fold_in(own, 4), (number_of // 2,), 0, 1 << 20) % (room + 1)
    lengths = lengths.at[giver].add(-moved).at[receiver].add(moved)
    items = jnp.searchsorted(jnp.cumsum(lengths), jnp.arange(rows * top), side="right").astype(jnp.int32)
    grid = items.reshape(top, rows).T
    grid = grid[jax.random.permutation(jax.random.fold_in(own, 1), rows)]
    turn = jax.random.randint(jax.random.fold_in(own, 2), (rows, 1), 0, top)
    return jnp.take_along_axis(grid, (jnp.arange(top)[None, :] + turn) % top, axis=1)


def portions_of(number_of, total, bound, slope, full):
    weights = [(1 << 20) // math.isqrt(standing ** slope) + 1 for standing in range(1, number_of + 1)]
    largest = bound if full else min(bound, max(-(-total // number_of), total * weights[0] // sum(weights)))
    least = 1 if total - largest >= number_of - 1 else 0
    given, spare = [largest] + [least] * (number_of - 1), total - largest - least * (number_of - 1)
    while spare > 0:
        free = [i for i in range(1, number_of) if given[i] < largest] or [i for i in range(1, number_of) if given[i] < bound]
        whole, budget = sum([weights[i] for i in free]), spare
        for i in free:
            more = min(bound - given[i], max(1, budget * weights[i] // whole), spare)
            given[i] = given[i] + more
            spare = spare - more
    return np.array(given)


def centred(key, shape, spread, reach, pieces=(), kind=jnp.bfloat16):
    array = spread * jax.random.normal(key, shape, jnp.float32)
    if pieces:
        array = array * block_scale(key, shape, pieces, -0.22, 0.18)
    return jnp.clip(array, -reach, reach).astype(kind)


def setup_inputs(seed: int = 0, part: int = 0) -> dict:
    key_list = jax.random.split(jax.random.key(seed), 12)
    part_splits = jax.random.split(jax.random.fold_in(key_list[11], part), 12)
    item_features = centred(part_splits[0], (CAND, FEAT), 1.0, 6.0, ((0, 16),))
    tower_in = centred(key_list[1], (FEAT, TOWER), FEAT ** -0.5, 0.1875)
    tower_out = centred(key_list[2], (TOWER, D), TOWER ** -0.5, 0.125)
    proj_weight = centred(key_list[3], (D, 4 * D), D ** -0.5, 0.25)
    out_weight = centred(key_list[4], (D, D), D ** -0.5, 0.25)
    hist_keys = centred(part_splits[5], (USERS, HIST, D), 1.0, 6.0, ((1, 16),))
    hist_values = centred(part_splits[6], (USERS, HIST, D), 1.0, 6.0, ((1, 16),))
    owner_of_keys = jax.random.split(jax.random.fold_in(part_splits[7], 1), CPS * USERS // (CPS_DEV * USERS))
    owner_of_turns = jax.random.permutation(jax.random.fold_in(part_splits[7], 3), CPS * USERS // (CPS_DEV * USERS))
    owner_of = jax.vmap(lambda own, number: assign_block(jax.random.fold_in(part_splits[7], 2), own, number, CPS_DEV * USERS, N_SEQ, 1, MOST, 2))(owner_of_keys, owner_of_turns).reshape((CPS, USERS, 1))
    row_in = with_ends(jax.random.randint(part_splits[8], (CPS, USERS), 0, CAND_DEV), jax.random.fold_in(part_splits[8], 1), 0, CAND_DEV - 1).astype(jnp.int32)
    hist_lengths = jax.random.randint(part_splits[9], (USERS,), HIST // 4, HIST + 1).astype(jnp.int32)
    causal_offsets = with_ends(jax.random.randint(part_splits[10], (CPS, USERS), 0, HIST_DEV), jax.random.fold_in(part_splits[10], 1), 0, HIST_DEV - 1).astype(jnp.int32)
    return dict(item_features=item_features, tower_in=tower_in, tower_out=tower_out, proj_weight=proj_weight, out_weight=out_weight, hist_keys=hist_keys, hist_values=hist_values, owner_of=owner_of, row_in=row_in, hist_lengths=hist_lengths, causal_offsets=causal_offsets)


def layer_norm(values):
    centre = values - lax.optimization_barrier(jnp.mean(values, axis=-1, keepdims=True))
    return centre * lax.rsqrt(lax.optimization_barrier(jnp.mean(centre * centre, axis=-1, keepdims=True)) + 1e-05)

def self_term(query, key, value):
    rows = query.shape[0]
    size = D // HEADS
    q_heads = query.astype(jnp.float32).reshape(rows, HEADS, size)
    k_heads = key.astype(jnp.float32).reshape(rows, HEADS, size)
    v_heads = value.astype(jnp.float32).reshape(rows, HEADS, size)
    score = lax.optimization_barrier(jnp.sum(q_heads * k_heads, axis=-1)) * size ** (-0.5)
    return (jax.nn.silu(score)[:, :, None] * v_heads).reshape(rows, D)

def attend_block(query, keys, values, visible):
    rows = query.shape[0]
    size = D // HEADS
    q_heads = query.astype(jnp.float32).reshape(rows, HEADS, size)
    k_heads = keys.astype(jnp.float32).reshape(keys.shape[0], HEADS, size)
    v_heads = values.astype(jnp.float32).reshape(values.shape[0], HEADS, size)
    scores = jnp.einsum('chd,jhd->hcj', q_heads, k_heads, precision=lax.Precision.HIGHEST) * size ** (-0.5)
    weights = jnp.where(visible[None], jax.nn.silu(scores), 0.0).astype(jnp.bfloat16)
    mixed = jnp.einsum('hcj,jhd->chd', weights.astype(jnp.float32), v_heads, precision=lax.Precision.HIGHEST)
    return mixed.reshape(rows, D)

def user_attention(operands):
    query, keys, values, limit = operands
    key_blocks = keys.reshape(N_SEQ, HIST_DEV, D)
    value_blocks = values.reshape(N_SEQ, HIST_DEV, D)

    def step(total, block):
        index, key_block, value_block = block
        positions = index * HIST_DEV + jnp.arange(HIST_DEV, dtype=jnp.int32)
        visible = positions[None, :] < limit[:, None]
        return (total + attend_block(query, key_block, value_block, visible), None)
    start = jnp.zeros((CPS, D), jnp.float32)
    total, _ = lax.scan(step, start, (jnp.arange(N_SEQ, dtype=jnp.int32), key_blocks, value_blocks))
    return total

def reference(item_features, tower_in, tower_out, proj_weight, out_weight, hist_keys, hist_values, owner_of, row_in, hist_lengths, causal_offsets):
    hidden = jax.nn.silu(jnp.dot(item_features, tower_in, preferred_element_type=jnp.float32)).astype(jnp.bfloat16)
    item_embed = jnp.dot(hidden, tower_out, preferred_element_type=jnp.float32).astype(jnp.bfloat16)
    pool = (owner_of[:, :, 0].astype(jnp.int32) * CAND_DEV + row_in.astype(jnp.int32)).reshape(-1)
    routed = jnp.take(item_embed, pool, axis=0)
    proj = jax.nn.silu(jnp.dot(routed, proj_weight, preferred_element_type=jnp.float32))
    gate = proj[:, :D]
    value = proj[:, D:2 * D].astype(jnp.bfloat16)
    query = proj[:, 2 * D:3 * D].astype(jnp.bfloat16)
    key = proj[:, 3 * D:].astype(jnp.bfloat16)
    own = self_term(query, key, value)
    query_users = query.reshape(CPS, USERS, D).transpose(1, 0, 2)
    limits = (hist_lengths[None, :] - causal_offsets).T
    attended = lax.map(user_attention, (query_users, hist_keys, hist_values, limits))
    total = attended.transpose(1, 0, 2).reshape(CPS * USERS, D) + own
    mixed = (layer_norm(total) * gate).astype(jnp.bfloat16)
    result = routed.astype(jnp.float32) + jnp.dot(mixed, out_weight, preferred_element_type=jnp.float32)
    return (item_embed, result.astype(jnp.bfloat16).reshape(CPS, USERS, D))
```

```python
import functools
import jax
import jax.numpy as jnp
from jax import lax
from jax.experimental import pallas as pl
from jax.experimental.pallas import tpu as pltpu
from jax.sharding import PartitionSpec as P

HEADS = 8
CORES = 2
F32 = jnp.float32
BF16 = jnp.bfloat16
MESH = pl.DeviceIdType.MESH


def silu(x):
    half = 0.5 * x
    return half + half * jnp.tanh(half)


def dot(a, b):
    return jnp.dot(a, b, preferred_element_type=F32)


def hot(mask):
    return jnp.where(mask, 1.0, 0.0)


def lanes(shape):
    return lax.broadcasted_iota(jnp.int32, shape, 1)


def rows_of(shape):
    return lax.broadcasted_iota(jnp.int32, shape, 0)


def kernel(
    n,
    depth,
    ids_ref,
    off_ref,
    lens_ref,
    feat_hbm,
    tin_hbm,
    tout_hbm,
    proj_hbm,
    outw_hbm,
    keys_hbm,
    vals_hbm,
    embed_out,
    cand_out,
    feat_v,
    tin_v,
    tout_v,
    proj_v,
    outw_v,
    k_v,
    v_v,
    eflat,
    sflat,
    ebuf,
    erecv,
    sbuf,
    rrecv,
    qbuf,
    qall,
    pbuf,
    precv,
    own_v,
    gate_v,
    routed_v,
    load_sem,
    tin_sem,
    tout_sem,
    kv_send,
    kv_recv,
    e_send,
    e_recv,
    s_send,
    s_recv,
    q_send,
    q_recv,
    p_send,
    p_recv,
):
    me = lax.axis_index("seq")
    core = lax.rem(me, CORES)
    partner = me + 1 - 2 * core
    users, cands, width = qbuf.shape
    slots = users * cands
    item_rows = embed_out.shape[0]
    chunks = tin_v.shape[0]
    tile = tin_v.shape[2]

    def remote(src, dst, send, recv, device):
        return pltpu.make_async_remote_copy(
            src_ref=src,
            dst_ref=dst,
            send_sem=send,
            recv_sem=recv,
            device_id={"seq": device},
            device_id_type=MESH,
        )

    def each_peer(act):
        def step(j, carry):
            act(lax.rem(me + j, n))
            return carry

        lax.fori_loop(1, n, step, 0)

    barrier = pltpu.get_barrier_semaphore()
    each_peer(
        lambda peer: pl.semaphore_signal(
            barrier, inc=1, device_id={"seq": peer}, device_id_type=MESH
        )
    )

    feat_load = pltpu.make_async_copy(feat_hbm, feat_v, load_sem.at[0])
    feat_load.start()
    tin_load = [
        pltpu.make_async_copy(
            tin_hbm.at[:, pl.ds(j * tile, tile)], tin_v.at[j], tin_sem.at[j]
        )
        for j in range(chunks)
    ]
    tout_load = [
        pltpu.make_async_copy(
            tout_hbm.at[pl.ds(j * tile, tile), :], tout_v.at[j], tout_sem.at[j]
        )
        for j in range(chunks)
    ]
    for j in range(chunks):
        tin_load[j].start()
        tout_load[j].start()

    owner_row = ids_ref[0:1, :].astype(F32)
    item_row = ids_ref[1:2, :].astype(F32)
    square = (slots, slots)
    first, second = rows_of(square), lanes(square)
    owner_wide = jnp.broadcast_to(owner_row, square)
    item_wide = jnp.broadcast_to(item_row, square)
    owner_col = jnp.sum(jnp.where(first == second, owner_wide, 0.0), axis=1, keepdims=True)
    item_col = jnp.sum(jnp.where(first == second, item_wide, 0.0), axis=1, keepdims=True)
    same = hot(owner_wide == owner_col)
    rank_col = jnp.sum(jnp.where(second < first, same, 0.0), axis=1, keepdims=True)
    rank_row = jnp.sum(jnp.where(first < second, same, 0.0), axis=0, keepdims=True)
    code_col = owner_col * depth + rank_col
    code_row = owner_row * depth + rank_row
    home = hot(lanes((slots, n * depth)).astype(F32) == code_col).astype(BF16)
    away = hot(rows_of((n * depth, slots)).astype(F32) == code_row).astype(BF16)
    picks = hot(lanes((slots, item_rows)).astype(F32) == item_col).astype(BF16)
    eflat[...] = dot(away, picks)
    for d in range(n):
        ebuf[d] = eflat[d * depth : (d + 1) * depth, :].astype(BF16)

    pl.semaphore_wait(barrier, n - 1)

    each_peer(
        lambda peer: remote(
            ebuf.at[peer], erecv.at[me], e_send.at[peer], e_recv.at[me], peer
        ).start()
    )
    erecv[me] = ebuf[me]

    def history(held, full, number):
        return (
            remote(held.at[1 - core], full.at[core], kv_send.at[number], kv_recv.at[number], partner),
            pltpu.make_async_copy(held.at[core], full.at[core], load_sem.at[3 + number]),
        )

    proj_load = pltpu.make_async_copy(proj_hbm, proj_v, load_sem.at[1])
    outw_load = pltpu.make_async_copy(outw_hbm, outw_v, load_sem.at[2])
    key_moves = history(keys_hbm, k_v, 0)
    value_moves = history(vals_hbm, v_v, 1)
    proj_load.start()
    for move in key_moves + value_moves:
        move.start()
    outw_load.start()

    feat_load.wait()
    embed = jnp.zeros((item_rows, width), F32)
    for j in range(chunks):
        tin_load[j].wait()
        hidden = silu(dot(feat_v[...], tin_v[j])).astype(BF16)
        tout_load[j].wait()
        embed = embed + dot(hidden, tout_v[j])
    embed = embed.astype(BF16)
    embed_out[...] = embed

    each_peer(
        lambda peer: remote(
            ebuf.at[peer], erecv.at[peer], e_send.at[peer], e_recv.at[peer], peer
        ).wait_recv()
    )
    for d in range(n):
        eflat[d * depth : (d + 1) * depth, :] = erecv[d].astype(F32)
    sflat[...] = dot(eflat[...].astype(BF16), embed)
    for d in range(n):
        sbuf[d] = sflat[d * depth : (d + 1) * depth, :].astype(BF16)
    each_peer(
        lambda peer: remote(
            sbuf.at[peer], rrecv.at[me], s_send.at[peer], s_recv.at[me], peer
        ).start()
    )
    rrecv[me] = sbuf[me]
    proj_load.wait()
    each_peer(
        lambda peer: remote(
            sbuf.at[peer], rrecv.at[peer], s_send.at[peer], s_recv.at[peer], peer
        ).wait_recv()
    )
    for d in range(n):
        sflat[d * depth : (d + 1) * depth, :] = rrecv[d].astype(F32)
    routed = dot(home, sflat[...].astype(BF16))
    routed_v[...] = routed
    routed = routed.astype(BF16)
    query = silu(dot(routed, proj_v[:, 2 * width : 3 * width])).astype(BF16)
    for u in range(users):
        qbuf[u] = query[u * cands : (u + 1) * cands, :]
    each_peer(
        lambda peer: remote(
            qbuf.at[lax.rem(peer, CORES)], qall.at[me], q_send.at[peer], q_recv.at[me], peer
        ).start()
    )
    qall[me] = qbuf[core]

    size = width // HEADS
    gate_v[...] = silu(dot(routed, proj_v[:, :width]))
    value = silu(dot(routed, proj_v[:, width : 2 * width])).astype(BF16)
    key = silu(dot(routed, proj_v[:, 3 * width :])).astype(BF16)
    products = query.astype(F32) * key.astype(F32)
    wide = (width, width)
    blocks = hot(rows_of(wide) // size == lanes(wide) // size)
    score = jnp.dot(
        products, blocks, preferred_element_type=F32, precision=lax.Precision.HIGHEST
    ) * size ** (-0.5)
    own_v[...] = silu(score) * value.astype(F32)

    for move in key_moves + value_moves:
        pass
    for local in (key_moves[1], value_moves[1]):
        local.wait()
    for held, full, number in ((keys_hbm, k_v, 0), (vals_hbm, v_v, 1)):
        remote(
            held.at[1 - core], full.at[1 - core], kv_send.at[number], kv_recv.at[number], partner
        ).wait_recv()

    events = k_v.shape[1]
    quad = min(width, 256)
    quad_heads = quad // size
    pack = max(1, 256 // (quad_heads * cands))
    while n % pack:
        pack -= 1
    turns = n // pack
    queries = pack * cands
    tall = quad_heads * queries
    span = min(events, 512)
    base = (me // CORES) * CORES * events
    length = lens_ref[core]
    block_mask = rows_of((tall, quad)) // queries == lanes((tall, quad)) // size

    def turn(t, carry):
        block = lax.rem(me // pack + t, turns)
        for i in range(pack):
            source = block * pack + i

            @pl.when(source != me)
            def _():
                remote(
                    qbuf.at[0], qall.at[source], q_send.at[source], q_recv.at[source], source
                ).wait_recv()

        offsets = off_ref[pl.ds(block * queries, queries), :]
        offset = jnp.sum(
            jnp.where(lanes((queries, users)) == core, offsets, 0), axis=1, keepdims=True
        )
        limit = length - base - offset
        limit = jnp.concatenate([limit] * quad_heads, axis=0)
        packed = qall[pl.ds(block * pack, pack)].reshape(queries, width).astype(F32)
        packed = packed * (0.5 * size ** (-0.5))
        for part in range(width // quad):
            columns = slice(part * quad, (part + 1) * quad)
            spread = jnp.concatenate([packed[:, columns]] * quad_heads, axis=0)
            spread = jnp.where(block_mask, spread, 0.0).astype(BF16)
            total = jnp.zeros((tall, quad), F32)
            for half in range(CORES):
                for start in range(0, events, span):
                    keys = k_v[half, start : start + span, columns]
                    score = lax.dot_general(
                        spread, keys, (((1,), (1,)), ((), ())), preferred_element_type=F32
                    )
                    seen = lanes((tall, span)) < limit - (half * events + start)
                    weight = jnp.where(seen, score + score * jnp.tanh(score), 0.0)
                    total = total + dot(
                        weight.astype(BF16), v_v[half, start : start + span, columns]
                    )
            total = jnp.where(block_mask, total, 0.0)
            mixed = total[:queries]
            for head in range(1, quad_heads):
                mixed = mixed + total[head * queries : (head + 1) * queries]
            pbuf[pl.ds(block * pack, pack), :, columns] = mixed.astype(BF16).reshape(
                pack, cands, quad
            )
        for i in range(pack):
            target = block * pack + i

            @pl.when(target != me)
            def _():
                remote(
                    pbuf.at[target], precv.at[me], p_send.at[target], p_recv.at[me], target
                ).start()

        return carry

    lax.fori_loop(0, turns, turn, 0)
    precv[me] = pbuf[me]
    outw_load.wait()
    each_peer(
        lambda peer: remote(
            pbuf.at[peer], precv.at[peer], p_send.at[peer], p_recv.at[peer], peer
        ).wait_recv()
    )
    sums = []
    for u in range(users):
        total = precv[u].astype(F32)
        for d in range(u + CORES, n, CORES):
            total = total + precv[d].astype(F32)
        sums.append(total)
    total = jnp.concatenate(sums, axis=0) + own_v[...]
    centre = total - jnp.mean(total, axis=-1, keepdims=True)
    scale = lax.rsqrt(jnp.mean(centre * centre, axis=-1, keepdims=True) + 1e-05)
    mixed = (centre * scale * gate_v[...]).astype(BF16)
    cand_out[...] = (routed_v[...] + dot(mixed, outw_v[...])).astype(BF16)

    def finish(peer):
        remote(ebuf.at[peer], erecv.at[peer], e_send.at[peer], e_recv.at[peer], peer).wait_send()
        remote(sbuf.at[peer], rrecv.at[peer], s_send.at[peer], s_recv.at[peer], peer).wait_send()
        remote(qbuf.at[0], qall.at[peer], q_send.at[peer], q_recv.at[peer], peer).wait_send()
        remote(pbuf.at[peer], precv.at[peer], p_send.at[peer], p_recv.at[peer], peer).wait_send()

    each_peer(finish)
    key_moves[0].wait_send()
    value_moves[0].wait_send()


def per_device(
    item_features,
    tower_in,
    tower_out,
    proj_weight,
    out_weight,
    hist_keys,
    hist_values,
    owner_of,
    row_in,
    hist_lengths,
    causal_offsets,
):
    n = lax.axis_size("seq")
    cands, users = row_in.shape
    slots = cands * users
    depth = max(2, 2 * slots // n)
    item_rows, features = item_features.shape
    tower, width = tower_out.shape
    events = hist_keys.shape[1]
    tile = min(tower, 512)
    ids = jnp.stack([owner_of[:, :, 0].T.reshape(slots), row_in.T.reshape(slots)])
    vmem = pl.BlockSpec(memory_space=pltpu.VMEM)
    smem = pl.BlockSpec(memory_space=pltpu.SMEM)
    anywhere = pl.BlockSpec(memory_space=pl.ANY)
    dma = pltpu.SemaphoreType.DMA
    item_embed, cand_out = pl.pallas_call(
        functools.partial(kernel, n, depth),
        out_shape=(
            jax.ShapeDtypeStruct((item_rows, width), BF16),
            jax.ShapeDtypeStruct((slots, width), BF16),
        ),
        in_specs=[vmem, vmem, smem] + [anywhere] * 7,
        out_specs=(vmem, vmem),
        scratch_shapes=[
            pltpu.VMEM((item_rows, features), BF16),
            pltpu.VMEM((tower // tile, features, tile), BF16),
            pltpu.VMEM((tower // tile, tile, width), BF16),
            pltpu.VMEM(proj_weight.shape, BF16),
            pltpu.VMEM(out_weight.shape, BF16),
            pltpu.VMEM((CORES, events, width), BF16),
            pltpu.VMEM((CORES, events, width), BF16),
            pltpu.VMEM((n * depth, item_rows), F32),
            pltpu.VMEM((n * depth, width), F32),
            pltpu.VMEM((n, depth, item_rows), BF16),
            pltpu.VMEM((n, depth, item_rows), BF16),
            pltpu.VMEM((n, depth, width), BF16),
            pltpu.VMEM((n, depth, width), BF16),
            pltpu.VMEM((users, cands, width), BF16),
            pltpu.VMEM((n, cands, width), BF16),
            pltpu.VMEM((n, cands, width), BF16),
            pltpu.VMEM((n, cands, width), BF16),
            pltpu.VMEM((slots, width), F32),
            pltpu.VMEM((slots, width), F32),
            pltpu.VMEM((slots, width), F32),
            dma((5,)),
            dma((tower // tile,)),
            dma((tower // tile,)),
            dma((2,)),
            dma((2,)),
        ]
        + [dma((n,))] * 8,
        compiler_params=pltpu.CompilerParams(collective_id=0, has_side_effects=True),
    )(
        ids,
        causal_offsets,
        hist_lengths,
        item_features,
        tower_in,
        tower_out,
        proj_weight,
        out_weight,
        hist_keys,
        hist_values,
    )
    return (item_embed, cand_out.reshape(users, cands, width).transpose(1, 0, 2))


def solution(mesh):
    return jax.shard_map(
        per_device,
        mesh=mesh,
        in_specs=(
            P(("grp", "seq"), None),
            P(),
            P(),
            P(),
            P(),
            P("grp", "seq", None),
            P("grp", "seq", None),
            P(("grp", "seq"), None, None),
            P(("grp", "seq"), None),
            P("grp"),
            P("grp", None),
        ),
        out_specs=(P(("grp", "seq"), None), P(("grp", "seq"), None, None)),
        check_vma=False,
    )
```

```python
import functools
import jax
import jax.numpy as jnp
from jax import lax
from jax.experimental import pallas as pl
from jax.experimental.pallas import tpu as pltpu
from jax.sharding import PartitionSpec as P

HEADS = 8
CORES = 2
F32 = jnp.float32
BF16 = jnp.bfloat16
MESH = pl.DeviceIdType.MESH


def silu(x):
    half = 0.5 * x
    return half + half * jnp.tanh(half)


def dot(a, b):
    return jnp.dot(a, b, preferred_element_type=F32)


def hot(mask):
    return jnp.where(mask, 1.0, 0.0)


def lanes(shape):
    return lax.broadcasted_iota(jnp.int32, shape, 1)


def rows_of(shape):
    return lax.broadcasted_iota(jnp.int32, shape, 0)


def kernel(
    n,
    depth,
    owner_ref,
    item_ref,
    off_ref,
    lens_ref,
    feat_hbm,
    tin_hbm,
    tout_hbm,
    proj_hbm,
    outw_hbm,
    keys_hbm,
    vals_hbm,
    embed_out,
    cand_out,
    feat_v,
    tin_v,
    tout_v,
    proj_v,
    outw_v,
    k_v,
    v_v,
    eflat,
    sflat,
    ebuf,
    erecv,
    sbuf,
    rrecv,
    qbuf,
    qall,
    pbuf,
    precv,
    own_v,
    limit_v,
    gate_v,
    routed_v,
    load_sem,
    tin_sem,
    tout_sem,
    kv_send,
    kv_recv,
    e_send,
    e_recv,
    s_send,
    s_recv,
    q_send,
    q_recv,
    p_send,
    p_recv,
):
    me = lax.axis_index("seq")
    core = lax.rem(me, CORES)
    partner = me + 1 - 2 * core
    users, cands, width = qbuf.shape
    slots = users * cands
    item_rows = embed_out.shape[0]
    chunks = tin_v.shape[0]
    tile = tin_v.shape[2]

    def remote(src, dst, send, recv, device):
        return pltpu.make_async_remote_copy(
            src_ref=src,
            dst_ref=dst,
            send_sem=send,
            recv_sem=recv,
            device_id={"seq": device},
            device_id_type=MESH,
        )

    def each_peer(act, sign=1):
        def step(j, carry):
            act(lax.rem(me + n + sign * j, n))
            return carry

        lax.fori_loop(1, n, step, 0)

    barrier = pltpu.get_barrier_semaphore()
    each_peer(
        lambda peer: pl.semaphore_signal(
            barrier, inc=1, device_id={"seq": peer}, device_id_type=MESH
        )
    )

    feat_load = pltpu.make_async_copy(feat_hbm, feat_v, load_sem.at[0])
    feat_load.start()
    tin_load = [
        pltpu.make_async_copy(
            tin_hbm.at[:, pl.ds(j * tile, tile)], tin_v.at[j], tin_sem.at[j]
        )
        for j in range(chunks)
    ]
    tout_load = [
        pltpu.make_async_copy(
            tout_hbm.at[pl.ds(j * tile, tile), :], tout_v.at[j], tout_sem.at[j]
        )
        for j in range(chunks)
    ]
    for j in range(chunks):
        tin_load[j].start()
        tout_load[j].start()

    def as_row(ref):
        return jnp.concatenate([ref[u : u + 1, :] for u in range(users)], axis=1).astype(F32)

    owner_row, item_row = as_row(owner_ref), as_row(item_ref)
    square = (slots, slots)
    first, second = rows_of(square), lanes(square)
    owner_wide = jnp.broadcast_to(owner_row, square)
    item_wide = jnp.broadcast_to(item_row, square)
    owner_col = jnp.sum(jnp.where(first == second, owner_wide, 0.0), axis=1, keepdims=True)
    item_col = jnp.sum(jnp.where(first == second, item_wide, 0.0), axis=1, keepdims=True)
    same = hot(owner_wide == owner_col)
    rank_col = jnp.sum(jnp.where(second < first, same, 0.0), axis=1, keepdims=True)
    rank_row = jnp.sum(jnp.where(first < second, same, 0.0), axis=0, keepdims=True)
    code_col = owner_col * depth + rank_col
    code_row = owner_row * depth + rank_row
    home = hot(lanes((slots, n * depth)).astype(F32) == code_col).astype(BF16)
    away = hot(rows_of((n * depth, slots)).astype(F32) == code_row).astype(BF16)
    picks = hot(lanes((slots, item_rows)).astype(F32) == item_col).astype(BF16)
    eflat[...] = dot(away, picks)
    for d in range(n):
        ebuf[d] = eflat[d * depth : (d + 1) * depth, :].astype(BF16)

    candidates = limit_v.shape[0]
    offset_row = jnp.sum(
        jnp.where(rows_of((users, candidates)) == core, off_ref[...], 0), axis=0, keepdims=True
    )
    for start in range(0, candidates, 256):
        block = (min(256, candidates - start), candidates)
        offset = jnp.where(rows_of(block) + start == lanes(block), offset_row, 0)
        limit_v[start : start + block[0], :] = lens_ref[core] - jnp.sum(
            offset, axis=1, keepdims=True
        )

    pl.semaphore_wait(barrier, n - 1)

    each_peer(
        lambda peer: remote(
            ebuf.at[peer], erecv.at[me], e_send.at[peer], e_recv.at[me], peer
        ).start()
    )
    erecv[me] = ebuf[me]

    def history(held, full, number):
        return (
            remote(held.at[1 - core], full.at[core], kv_send.at[number], kv_recv.at[number], partner),
            pltpu.make_async_copy(held.at[core], full.at[core], load_sem.at[3 + number]),
        )

    proj_load = pltpu.make_async_copy(proj_hbm, proj_v, load_sem.at[1])
    outw_load = pltpu.make_async_copy(outw_hbm, outw_v, load_sem.at[2])
    key_moves = history(keys_hbm, k_v, 0)
    value_moves = history(vals_hbm, v_v, 1)
    feat_load.wait()
    embed = jnp.zeros((item_rows, width), F32)
    for j in range(chunks):
        tin_load[j].wait()
        hidden = silu(dot(feat_v[...], tin_v[j])).astype(BF16)
        tout_load[j].wait()
        if j == chunks - 1:
            proj_load.start()
            for move in key_moves + value_moves:
                move.start()
            outw_load.start()
        embed = embed + dot(hidden, tout_v[j])
    embed = embed.astype(BF16)
    embed_out[...] = embed

    each_peer(
        lambda peer: remote(
            ebuf.at[peer], erecv.at[peer], e_send.at[peer], e_recv.at[peer], peer
        ).wait_recv()
    )
    for d in range(n):
        eflat[d * depth : (d + 1) * depth, :] = erecv[d].astype(F32)
    sflat[...] = dot(eflat[...].astype(BF16), embed)
    for d in range(n):
        sbuf[d] = sflat[d * depth : (d + 1) * depth, :].astype(BF16)
    each_peer(
        lambda peer: remote(
            sbuf.at[peer], rrecv.at[me], s_send.at[peer], s_recv.at[me], peer
        ).start()
    )
    rrecv[me] = sbuf[me]
    proj_load.wait()
    each_peer(
        lambda peer: remote(
            sbuf.at[peer], rrecv.at[peer], s_send.at[peer], s_recv.at[peer], peer
        ).wait_recv()
    )
    for d in range(n):
        sflat[d * depth : (d + 1) * depth, :] = rrecv[d].astype(F32)
    routed = dot(home, sflat[...].astype(BF16))
    routed_v[...] = routed
    routed = routed.astype(BF16)
    query = silu(dot(routed, proj_v[:, 2 * width : 3 * width])).astype(BF16)
    for u in range(users):
        qbuf[u] = query[u * cands : (u + 1) * cands, :]
    each_peer(
        lambda peer: remote(
            qbuf.at[lax.rem(peer, CORES)], qall.at[me], q_send.at[peer], q_recv.at[me], peer
        ).start(),
        -1,
    )
    qall[me] = qbuf[core]

    size = width // HEADS
    gate_v[...] = silu(dot(routed, proj_v[:, :width]))
    value = silu(dot(routed, proj_v[:, width : 2 * width])).astype(BF16)
    key = silu(dot(routed, proj_v[:, 3 * width :])).astype(BF16)
    products = query.astype(F32) * key.astype(F32)
    wide = (width, width)
    blocks = hot(rows_of(wide) // size == lanes(wide) // size)
    score = jnp.dot(
        products, blocks, preferred_element_type=F32, precision=lax.Precision.HIGHEST
    ) * size ** (-0.5)
    own_v[...] = silu(score) * value.astype(F32)

    for local in (key_moves[1], value_moves[1]):
        local.wait()
    for held, full, number in ((keys_hbm, k_v, 0), (vals_hbm, v_v, 1)):
        remote(
            held.at[1 - core], full.at[1 - core], kv_send.at[number], kv_recv.at[number], partner
        ).wait_recv()

    events = k_v.shape[1]
    quad = min(width, 256)
    quad_heads = quad // size
    pack = max(1, 256 // (quad_heads * cands))
    while n % pack:
        pack -= 1
    turns = n // pack
    queries = pack * cands
    tall = quad_heads * queries
    span = min(events, 512)
    base = (me // CORES) * CORES * events
    block_mask = rows_of((tall, quad)) // queries == lanes((tall, quad)) // size

    def turn(t, carry):
        block = lax.rem(me // pack + t, turns)
        for i in range(pack):
            source = block * pack + i

            @pl.when(source != me)
            def _():
                remote(
                    qbuf.at[0], qall.at[source], q_send.at[source], q_recv.at[source], source
                ).wait_recv()

        limit = limit_v[pl.ds(block * queries, queries), :] - base
        limit = jnp.concatenate([limit] * quad_heads, axis=0)
        packed = qall[pl.ds(block * pack, pack)].reshape(queries, width).astype(F32)
        packed = packed * (0.5 * size ** (-0.5))
        for part in range(width // quad):
            columns = slice(part * quad, (part + 1) * quad)
            spread = jnp.concatenate([packed[:, columns]] * quad_heads, axis=0)
            spread = jnp.where(block_mask, spread, 0.0).astype(BF16)
            total = jnp.zeros((tall, quad), F32)
            for half in range(CORES):
                for start in range(0, events, span):
                    keys = k_v[half, start : start + span, columns]
                    score = lax.dot_general(
                        spread, keys, (((1,), (1,)), ((), ())), preferred_element_type=F32
                    )
                    seen = lanes((tall, span)) < limit - (half * events + start)
                    weight = jnp.where(seen, score + score * jnp.tanh(score), 0.0)
                    total = total + dot(
                        weight.astype(BF16), v_v[half, start : start + span, columns]
                    )
            total = jnp.where(block_mask, total, 0.0)
            mixed = total[:queries]
            for head in range(1, quad_heads):
                mixed = mixed + total[head * queries : (head + 1) * queries]
            pbuf[pl.ds(block * pack, pack), :, columns] = mixed.astype(BF16).reshape(
                pack, cands, quad
            )
        for i in range(pack):
            target = block * pack + i

            @pl.when(target != me)
            def _():
                remote(
                    pbuf.at[target], precv.at[me], p_send.at[target], p_recv.at[me], target
                ).start()

        return carry

    lax.fori_loop(0, turns, turn, 0)
    precv[me] = pbuf[me]
    outw_load.wait()
    each_peer(
        lambda peer: remote(
            pbuf.at[peer], precv.at[peer], p_send.at[peer], p_recv.at[peer], peer
        ).wait_recv()
    )
    sums = []
    for u in range(users):
        total = precv[u].astype(F32)
        for d in range(u + CORES, n, CORES):
            total = total + precv[d].astype(F32)
        sums.append(total)
    total = jnp.concatenate(sums, axis=0) + own_v[...]
    centre = total - jnp.mean(total, axis=-1, keepdims=True)
    scale = lax.rsqrt(jnp.mean(centre * centre, axis=-1, keepdims=True) + 1e-05)
    mixed = (centre * scale * gate_v[...]).astype(BF16)
    routed_v[...] = routed_v[...] + dot(mixed, outw_v[...])
    for i in range(cands):
        rows = [routed_v[u * cands + i : u * cands + i + 1, :] for u in range(users)]
        cand_out[i] = jnp.concatenate(rows, axis=0).astype(BF16)

    def finish(peer):
        remote(ebuf.at[peer], erecv.at[peer], e_send.at[peer], e_recv.at[peer], peer).wait_send()
        remote(sbuf.at[peer], rrecv.at[peer], s_send.at[peer], s_recv.at[peer], peer).wait_send()
        remote(qbuf.at[0], qall.at[peer], q_send.at[peer], q_recv.at[peer], peer).wait_send()
        remote(pbuf.at[peer], precv.at[peer], p_send.at[peer], p_recv.at[peer], peer).wait_send()

    each_peer(finish)
    key_moves[0].wait_send()
    value_moves[0].wait_send()


def hand_over(embed_ref, cand_ref, embed_out, cand_out):
    embed_out[...] = embed_ref[...]
    cand_out[...] = cand_ref[...]


def per_device(
    item_features,
    tower_in,
    tower_out,
    proj_weight,
    out_weight,
    hist_keys,
    hist_values,
    owner_of,
    row_in,
    hist_lengths,
    causal_offsets,
):
    n = lax.axis_size("seq")
    cands, users = row_in.shape
    slots = cands * users
    depth = max(2, 2 * slots // n)
    item_rows, features = item_features.shape
    tower, width = tower_out.shape
    events = hist_keys.shape[1]
    tile = min(tower, 512)
    vmem = pl.BlockSpec(memory_space=pltpu.VMEM)
    smem = pl.BlockSpec(memory_space=pltpu.SMEM)
    anywhere = pl.BlockSpec(memory_space=pl.ANY)
    dma = pltpu.SemaphoreType.DMA
    item_embed, cand_out = pl.pallas_call(
        functools.partial(kernel, n, depth),
        out_shape=(
            jax.ShapeDtypeStruct((item_rows, width), BF16),
            jax.ShapeDtypeStruct((cands, users, width), BF16),
        ),
        in_specs=[vmem, vmem, vmem, smem] + [anywhere] * 7,
        out_specs=(vmem, vmem),
        scratch_shapes=[
            pltpu.VMEM((item_rows, features), BF16),
            pltpu.VMEM((tower // tile, features, tile), BF16),
            pltpu.VMEM((tower // tile, tile, width), BF16),
            pltpu.VMEM(proj_weight.shape, BF16),
            pltpu.VMEM(out_weight.shape, BF16),
            pltpu.VMEM((CORES, events, width), BF16),
            pltpu.VMEM((CORES, events, width), BF16),
            pltpu.VMEM((n * depth, item_rows), F32),
            pltpu.VMEM((n * depth, width), F32),
            pltpu.VMEM((n, depth, item_rows), BF16),
            pltpu.VMEM((n, depth, item_rows), BF16),
            pltpu.VMEM((n, depth, width), BF16),
            pltpu.VMEM((n, depth, width), BF16),
            pltpu.VMEM((users, cands, width), BF16),
            pltpu.VMEM((n, cands, width), BF16),
            pltpu.VMEM((n, cands, width), BF16),
            pltpu.VMEM((n, cands, width), BF16),
            pltpu.VMEM((slots, width), F32),
            pltpu.VMEM((n * cands, 1), jnp.int32),
            pltpu.VMEM((slots, width), F32),
            pltpu.VMEM((slots, width), F32),
            dma((5,)),
            dma((tower // tile,)),
            dma((tower // tile,)),
            dma((2,)),
            dma((2,)),
        ]
        + [dma((n,))] * 8,
        compiler_params=pltpu.CompilerParams(collective_id=0, has_side_effects=True),
    )(
        owner_of[:, :, 0].T,
        row_in.T,
        causal_offsets.T,
        hist_lengths,
        item_features,
        tower_in,
        tower_out,
        proj_weight,
        out_weight,
        hist_keys,
        hist_values,
    )
    return pl.pallas_call(
        hand_over,
        out_shape=(
            jax.ShapeDtypeStruct(item_embed.shape, BF16),
            jax.ShapeDtypeStruct(cand_out.shape, BF16),
        ),
        in_specs=[vmem, vmem],
        out_specs=(vmem, vmem),
    )(item_embed, cand_out)


def solution(mesh):
    return jax.shard_map(
        per_device,
        mesh=mesh,
        in_specs=(
            P(("grp", "seq"), None),
            P(),
            P(),
            P(),
            P(),
            P("grp", "seq", None),
            P("grp", "seq", None),
            P(("grp", "seq"), None, None),
            P(("grp", "seq"), None),
            P("grp"),
            P("grp", None),
        ),
        out_specs=(P(("grp", "seq"), None), P(("grp", "seq"), None, None)),
        check_vma=False,
    )
```

```python
import functools
import jax
import jax.numpy as jnp
from jax import lax
from jax.experimental import pallas as pl
from jax.experimental.pallas import tpu as pltpu
from jax.sharding import PartitionSpec as P

HEADS = 8
CORES = 2
F32 = jnp.float32
BF16 = jnp.bfloat16
MESH = pl.DeviceIdType.MESH


def silu(x):
    half = 0.5 * x
    return half + half * jnp.tanh(half)


def dot(a, b):
    return jnp.dot(a, b, preferred_element_type=F32)


def hot(mask):
    return jnp.where(mask, 1.0, 0.0)


def lanes(shape):
    return lax.broadcasted_iota(jnp.int32, shape, 1)


def rows_of(shape):
    return lax.broadcasted_iota(jnp.int32, shape, 0)


def kernel(
    n,
    depth,
    owner_ref,
    item_ref,
    off_ref,
    lens_ref,
    feat_hbm,
    tin_hbm,
    tout_hbm,
    proj_hbm,
    outw_hbm,
    keys_hbm,
    vals_hbm,
    embed_out,
    cand_out,
    feat_v,
    tin_v,
    tout_v,
    proj_v,
    outw_v,
    k_v,
    v_v,
    eflat,
    sflat,
    ebuf,
    erecv,
    sbuf,
    rrecv,
    qbuf,
    qall,
    pbuf,
    precv,
    own_v,
    limit_v,
    gate_v,
    routed_v,
    load_sem,
    tin_sem,
    tout_sem,
    kv_send,
    kv_recv,
    e_send,
    e_recv,
    s_send,
    s_recv,
    q_send,
    q_recv,
    p_send,
    p_recv,
):
    me = lax.axis_index("seq")
    core = lax.rem(me, CORES)
    partner = me + 1 - 2 * core
    users, cands, width = qbuf.shape
    slots = users * cands
    item_rows = embed_out.shape[0]
    chunks = tin_v.shape[0]
    tile = tin_v.shape[2]

    def remote(src, dst, send, recv, device):
        return pltpu.make_async_remote_copy(
            src_ref=src,
            dst_ref=dst,
            send_sem=send,
            recv_sem=recv,
            device_id={"seq": device},
            device_id_type=MESH,
        )

    def each_peer(act, sign=1):
        def step(j, carry):
            act(lax.rem(me + n + sign * j, n))
            return carry

        lax.fori_loop(1, n, step, 0)

    barrier = pltpu.get_barrier_semaphore()
    each_peer(
        lambda peer: pl.semaphore_signal(
            barrier, inc=1, device_id={"seq": peer}, device_id_type=MESH
        )
    )

    feat_load = pltpu.make_async_copy(feat_hbm, feat_v, load_sem.at[0])
    feat_load.start()
    tin_load = [
        pltpu.make_async_copy(
            tin_hbm.at[:, pl.ds(j * tile, tile)], tin_v.at[j], tin_sem.at[j]
        )
        for j in range(chunks)
    ]
    tout_load = [
        pltpu.make_async_copy(
            tout_hbm.at[pl.ds(j * tile, tile), :], tout_v.at[j], tout_sem.at[j]
        )
        for j in range(chunks)
    ]
    for j in range(chunks):
        tin_load[j].start()
        tout_load[j].start()

    def as_row(ref):
        return jnp.concatenate([ref[u : u + 1, :] for u in range(users)], axis=1).astype(F32)

    owner_row, item_row = as_row(owner_ref), as_row(item_ref)
    square = (slots, slots)
    first, second = rows_of(square), lanes(square)
    owner_wide = jnp.broadcast_to(owner_row, square)
    item_wide = jnp.broadcast_to(item_row, square)
    owner_col = jnp.sum(jnp.where(first == second, owner_wide, 0.0), axis=1, keepdims=True)
    item_col = jnp.sum(jnp.where(first == second, item_wide, 0.0), axis=1, keepdims=True)
    same = hot(owner_wide == owner_col)
    rank_col = jnp.sum(jnp.where(second < first, same, 0.0), axis=1, keepdims=True)
    rank_row = jnp.sum(jnp.where(first < second, same, 0.0), axis=0, keepdims=True)
    code_col = owner_col * depth + rank_col
    code_row = owner_row * depth + rank_row
    home = hot(lanes((slots, n * depth)).astype(F32) == code_col).astype(BF16)
    away = hot(rows_of((n * depth, slots)).astype(F32) == code_row).astype(BF16)
    picks = hot(lanes((slots, item_rows)).astype(F32) == item_col).astype(BF16)
    eflat[...] = dot(away, picks)
    for d in range(n):
        ebuf[d] = eflat[d * depth : (d + 1) * depth, :].astype(BF16)

    pl.semaphore_wait(barrier, n - 1)

    each_peer(
        lambda peer: remote(
            ebuf.at[peer], erecv.at[me], e_send.at[peer], e_recv.at[me], peer
        ).start()
    )
    erecv[me] = ebuf[me]

    def history(held, full, number):
        return (
            remote(held.at[1 - core], full.at[core], kv_send.at[number], kv_recv.at[number], partner),
            pltpu.make_async_copy(held.at[core], full.at[core], load_sem.at[3 + number]),
        )

    proj_load = pltpu.make_async_copy(proj_hbm, proj_v, load_sem.at[1])
    outw_load = pltpu.make_async_copy(outw_hbm, outw_v, load_sem.at[2])
    key_moves = history(keys_hbm, k_v, 0)
    value_moves = history(vals_hbm, v_v, 1)
    feat_load.wait()
    embed = jnp.zeros((item_rows, width), F32)
    for j in range(chunks):
        tin_load[j].wait()
        hidden = silu(dot(feat_v[...], tin_v[j])).astype(BF16)
        tout_load[j].wait()
        if j == chunks - 1:
            proj_load.start()
            for move in key_moves + value_moves:
                move.start()
            outw_load.start()
        embed = embed + dot(hidden, tout_v[j])
    embed = embed.astype(BF16)
    embed_out[...] = embed

    each_peer(
        lambda peer: remote(
            ebuf.at[peer], erecv.at[peer], e_send.at[peer], e_recv.at[peer], peer
        ).wait_recv()
    )
    for d in range(n):
        eflat[d * depth : (d + 1) * depth, :] = erecv[d].astype(F32)
    sflat[...] = dot(eflat[...].astype(BF16), embed)
    for d in range(n):
        sbuf[d] = sflat[d * depth : (d + 1) * depth, :].astype(BF16)
    each_peer(
        lambda peer: remote(
            sbuf.at[peer], rrecv.at[me], s_send.at[peer], s_recv.at[me], peer
        ).start()
    )
    rrecv[me] = sbuf[me]
    proj_load.wait()
    each_peer(
        lambda peer: remote(
            sbuf.at[peer], rrecv.at[peer], s_send.at[peer], s_recv.at[peer], peer
        ).wait_recv()
    )
    for d in range(n):
        sflat[d * depth : (d + 1) * depth, :] = rrecv[d].astype(F32)
    routed = dot(home, sflat[...].astype(BF16))
    routed_v[...] = routed
    routed = routed.astype(BF16)
    query = silu(dot(routed, proj_v[:, 2 * width : 3 * width])).astype(BF16)
    for u in range(users):
        qbuf[u] = query[u * cands : (u + 1) * cands, :]
    each_peer(
        lambda peer: remote(
            qbuf.at[lax.rem(peer, CORES)], qall.at[me], q_send.at[peer], q_recv.at[me], peer
        ).start(),
        -1,
    )
    qall[me] = qbuf[core]

    size = width // HEADS
    candidates = limit_v.shape[0]
    offset_row = jnp.sum(
        jnp.where(rows_of((users, candidates)) == core, off_ref[...], 0), axis=0, keepdims=True
    )
    for start in range(0, candidates, 256):
        block = (min(256, candidates - start), candidates)
        offset = jnp.where(rows_of(block) + start == lanes(block), offset_row, 0)
        limit_v[start : start + block[0], :] = lens_ref[core] - jnp.sum(
            offset, axis=1, keepdims=True
        )

    for local in (key_moves[1], value_moves[1]):
        local.wait()
    for held, full, number in ((keys_hbm, k_v, 0), (vals_hbm, v_v, 1)):
        remote(
            held.at[1 - core], full.at[1 - core], kv_send.at[number], kv_recv.at[number], partner
        ).wait_recv()

    events = k_v.shape[1]
    quad = min(width, 256)
    quad_heads = quad // size
    pack = max(1, 256 // (quad_heads * cands))
    while n % pack:
        pack -= 1
    turns = n // pack
    queries = pack * cands
    tall = quad_heads * queries
    span = min(events, 512)
    base = (me // CORES) * CORES * events
    block_mask = rows_of((tall, quad)) // queries == lanes((tall, quad)) // size

    way = jnp.where(2 * (me // pack) >= turns, 1, -1)

    def turn(t, carry):
        block = lax.rem(me // pack + turns + way * t, turns)
        for i in range(pack):
            source = block * pack + i

            @pl.when(source != me)
            def _():
                remote(
                    qbuf.at[0], qall.at[source], q_send.at[source], q_recv.at[source], source
                ).wait_recv()

        limit = limit_v[pl.ds(block * queries, queries), :] - base
        limit = jnp.concatenate([limit] * quad_heads, axis=0)
        packed = qall[pl.ds(block * pack, pack)].reshape(queries, width).astype(F32)
        packed = packed * (0.5 * size ** (-0.5))
        for part in range(width // quad):
            columns = slice(part * quad, (part + 1) * quad)
            spread = jnp.concatenate([packed[:, columns]] * quad_heads, axis=0)
            spread = jnp.where(block_mask, spread, 0.0).astype(BF16)
            total = jnp.zeros((tall, quad), F32)
            for half in range(CORES):
                for start in range(0, events, span):
                    keys = k_v[half, start : start + span, columns]
                    score = lax.dot_general(
                        spread, keys, (((1,), (1,)), ((), ())), preferred_element_type=F32
                    )
                    seen = lanes((tall, span)) < limit - (half * events + start)
                    weight = jnp.where(seen, score + score * jnp.tanh(score), 0.0)
                    total = total + dot(
                        weight.astype(BF16), v_v[half, start : start + span, columns]
                    )
            total = jnp.where(block_mask, total, 0.0)
            mixed = total[:queries]
            for head in range(1, quad_heads):
                mixed = mixed + total[head * queries : (head + 1) * queries]
            pbuf[pl.ds(block * pack, pack), :, columns] = mixed.astype(BF16).reshape(
                pack, cands, quad
            )
        for i in range(pack):
            target = block * pack + i

            @pl.when(target != me)
            def _():
                remote(
                    pbuf.at[target], precv.at[me], p_send.at[target], p_recv.at[me], target
                ).start()

        return carry

    lax.fori_loop(0, turns, turn, 0)
    precv[me] = pbuf[me]
    routed = routed_v[...].astype(BF16)
    query = jnp.concatenate([qbuf[u] for u in range(users)], axis=0)
    gate_v[...] = silu(dot(routed, proj_v[:, :width]))
    value = silu(dot(routed, proj_v[:, width : 2 * width])).astype(BF16)
    key = silu(dot(routed, proj_v[:, 3 * width :])).astype(BF16)
    products = query.astype(F32) * key.astype(F32)
    wide = (width, width)
    blocks = hot(rows_of(wide) // size == lanes(wide) // size)
    score = jnp.dot(
        products, blocks, preferred_element_type=F32, precision=lax.Precision.HIGHEST
    ) * size ** (-0.5)
    own_v[...] = silu(score) * value.astype(F32)


    def finish(peer):
        remote(ebuf.at[peer], erecv.at[peer], e_send.at[peer], e_recv.at[peer], peer).wait_send()
        remote(sbuf.at[peer], rrecv.at[peer], s_send.at[peer], s_recv.at[peer], peer).wait_send()
        remote(qbuf.at[0], qall.at[peer], q_send.at[peer], q_recv.at[peer], peer).wait_send()
        remote(pbuf.at[peer], precv.at[peer], p_send.at[peer], p_recv.at[peer], peer).wait_send()

    each_peer(finish)
    key_moves[0].wait_send()
    value_moves[0].wait_send()
    outw_load.wait()
    each_peer(
        lambda peer: remote(
            pbuf.at[peer], precv.at[peer], p_send.at[peer], p_recv.at[peer], peer
        ).wait_recv()
    )
    sums = []
    for u in range(users):
        total = precv[u].astype(F32)
        for d in range(u + CORES, n, CORES):
            total = total + precv[d].astype(F32)
        sums.append(total)
    total = jnp.concatenate(sums, axis=0) + own_v[...]
    centre = total - jnp.mean(total, axis=-1, keepdims=True)
    scale = lax.rsqrt(jnp.mean(centre * centre, axis=-1, keepdims=True) + 1e-05)
    mixed = (centre * scale * gate_v[...]).astype(BF16)
    routed_v[...] = routed_v[...] + dot(mixed, outw_v[...])
    for i in range(cands):
        rows = [routed_v[u * cands + i : u * cands + i + 1, :] for u in range(users)]
        cand_out[i] = jnp.concatenate(rows, axis=0).astype(BF16)


def hand_over(embed_ref, cand_ref, embed_out, cand_out):
    embed_out[...] = embed_ref[...]
    cand_out[...] = cand_ref[...]


def per_device(
    item_features,
    tower_in,
    tower_out,
    proj_weight,
    out_weight,
    hist_keys,
    hist_values,
    owner_of,
    row_in,
    hist_lengths,
    causal_offsets,
):
    n = lax.axis_size("seq")
    cands, users = row_in.shape
    slots = cands * users
    depth = max(2, 2 * slots // n)
    item_rows, features = item_features.shape
    tower, width = tower_out.shape
    events = hist_keys.shape[1]
    tile = min(tower, 512)
    vmem = pl.BlockSpec(memory_space=pltpu.VMEM)
    smem = pl.BlockSpec(memory_space=pltpu.SMEM)
    anywhere = pl.BlockSpec(memory_space=pl.ANY)
    dma = pltpu.SemaphoreType.DMA
    item_embed, cand_out = pl.pallas_call(
        functools.partial(kernel, n, depth),
        out_shape=(
            jax.ShapeDtypeStruct((item_rows, width), BF16),
            jax.ShapeDtypeStruct((cands, users, width), BF16),
        ),
        in_specs=[vmem, vmem, vmem, smem] + [anywhere] * 7,
        out_specs=(vmem, vmem),
        scratch_shapes=[
            pltpu.VMEM((item_rows, features), BF16),
            pltpu.VMEM((tower // tile, features, tile), BF16),
            pltpu.VMEM((tower // tile, tile, width), BF16),
            pltpu.VMEM(proj_weight.shape, BF16),
            pltpu.VMEM(out_weight.shape, BF16),
            pltpu.VMEM((CORES, events, width), BF16),
            pltpu.VMEM((CORES, events, width), BF16),
            pltpu.VMEM((n * depth, item_rows), F32),
            pltpu.VMEM((n * depth, width), F32),
            pltpu.VMEM((n, depth, item_rows), BF16),
            pltpu.VMEM((n, depth, item_rows), BF16),
            pltpu.VMEM((n, depth, width), BF16),
            pltpu.VMEM((n, depth, width), BF16),
            pltpu.VMEM((users, cands, width), BF16),
            pltpu.VMEM((n, cands, width), BF16),
            pltpu.VMEM((n, cands, width), BF16),
            pltpu.VMEM((n, cands, width), BF16),
            pltpu.VMEM((slots, width), F32),
            pltpu.VMEM((n * cands, 1), jnp.int32),
            pltpu.VMEM((slots, width), F32),
            pltpu.VMEM((slots, width), F32),
            dma((5,)),
            dma((tower // tile,)),
            dma((tower // tile,)),
            dma((2,)),
            dma((2,)),
        ]
        + [dma((n,))] * 8,
        compiler_params=pltpu.CompilerParams(collective_id=0, has_side_effects=True),
    )(
        owner_of[:, :, 0].T,
        row_in.T,
        causal_offsets.T,
        hist_lengths,
        item_features,
        tower_in,
        tower_out,
        proj_weight,
        out_weight,
        hist_keys,
        hist_values,
    )
    return pl.pallas_call(
        hand_over,
        out_shape=(
            jax.ShapeDtypeStruct(item_embed.shape, BF16),
            jax.ShapeDtypeStruct(cand_out.shape, BF16),
        ),
        in_specs=[vmem, vmem],
        out_specs=(vmem, vmem),
    )(item_embed, cand_out)


def solution(mesh):
    return jax.shard_map(
        per_device,
        mesh=mesh,
        in_specs=(
            P(("grp", "seq"), None),
            P(),
            P(),
            P(),
            P(),
            P("grp", "seq", None),
            P("grp", "seq", None),
            P(("grp", "seq"), None, None),
            P(("grp", "seq"), None),
            P("grp"),
            P("grp", None),
        ),
        out_specs=(P(("grp", "seq"), None), P(("grp", "seq"), None, None)),
        check_vma=False,
    )
```
